256 devices in a mesh: pipe: 8 (over x, z_lo), tensor: 4 (over y), expert: 8 (over z_hi, core).
Axes of the slice: x: 4, y: 4, z: 8 (z_hi: 4, z_lo: 2; z = z_hi * 2 + z_lo), core: 2. Of those that a mesh axis runs over, the one named last changes fastest.
Arguments:
- tokens: bfloat16 [2, 512, 4096], P(None, 'expert'), may hold values from -6 to 6
- gains: float32 [8, 4096], P('pipe'), may hold values from 0.1 to 1.9
- route_ids: int32 [8, 2, 512, 2], P('pipe', None, 'expert'), may hold values from 0 to 7, all different within a row
- route_weights: float32 [8, 2, 512, 2], P('pipe', None, 'expert'), may hold values from 0.2 to 1
- picks: int32 [8, 2, 8, 64], P('pipe', None, 'expert'), may hold values from 0 to 63, each once within a row
- w_gate: bfloat16 [8, 8, 4096, 1536], P('pipe', 'expert', None, 'tensor'), may hold values from -0.09375 to 0.09375
- w_up: bfloat16 [8, 8, 4096, 1536], P('pipe', 'expert', None, 'tensor'), may hold values from -0.09375 to 0.09375
- w_down: bfloat16 [8, 8, 1536, 4096], P('pipe', 'expert', 'tensor'), may hold values from -0.15625 to 0.15625
Outputs:
- streams: bfloat16 [8, 2, 512, 4096], P('pipe', None, 'expert', 'tensor')
The draws below stay inside these ranges and needn't reach their ends.
Inputs may be any that keep to these rules, and one draw needn't show every extreme that they name: `route_ids`: each token names 2 different experts; every expert is named by some token. `picks`: for every layer, micro-batch and block of 64 tokens, a permutation of 0 to 63.
All inputs are finite; a program needn't handle non-finite values.
Results may differ from the reference program's by a relative error of at most 0.025.
Values may be sent and summed in bfloat16 or wider, within the bound.
A program may use at most 64 MiB of HBM per device.

```python
import jax
import jax.numpy as jnp
from jax import lax

D = 4096
FF = 1536
TOPK = 2
MICRO = 2
TOK_DEV = 64
EXPERTS = 8
QUARTER = 16
CAP = 5
TOKENS = 512
N_PIPE = 8
N_TENSOR = 4
N_EXPERT = 8


def steps_of(rng, shape, shards, low, top_value):
    loudness, own = 1.0, jax.random.fold_in(rng, 6)
    for dim, parts in shards:
        steps = jnp.exp(jax.random.uniform(jax.random.fold_in(own, dim), (parts,), jnp.float32, low / len(shards), top_value / len(shards)))
        loudness = loudness * jnp.repeat(steps, shape[dim] // parts).reshape([-1 if axis == dim else 1 for axis in range(len(shape))])
    return loudness


def different_ones(stream_key, rows, number_of, top, lift):
    sequence = jax.random.permutation(jax.random.fold_in(stream_key, 1), number_of)
    pull = sequence
    for power in range(3):
        pull = pull * pull // number_of
    pull = pull * lift // number_of
    lots = jax.random.randint(jax.random.fold_in(stream_key, 2), (rows, number_of), 0, 4096) + pull
    fixed_rows = jax.random.permutation(jax.random.fold_in(stream_key, 3), rows)[jnp.arange(number_of) % rows]
    lots = jnp.where(jnp.arange(rows)[:, None] == fixed_rows[None, :], 1 << 14, lots)
    priority = lots * number_of + jnp.arange(number_of)
    return lax.top_k(priority.astype(jnp.int32), top)[1].astype(jnp.int32)


def gaussian(key, shape, deviation, most, pieces=(), kind=jnp.bfloat16):
    values = jax.random.normal(key, shape, jnp.float32) * deviation
    if len(pieces) > 0:
        values = steps_of(key, shape, pieces, -0.22, 0.18) * values
    return jnp.clip(values, min=-most, max=most).astype(kind)


def setup_inputs(seed: int = 0) -> dict:
    key_list = jax.random.split(jax.random.key(seed), 9)
    tokens = gaussian(key_list[0], (MICRO, TOKENS, D), 1.0, 6.0, ((1, 8),))
    gains = jnp.clip(1.0 + 0.18 * jax.random.normal(key_list[1], (N_PIPE, D), jnp.float32), 0.1, 1.9)
    route_ids = different_ones(key_list[2], N_PIPE * MICRO * TOKENS, EXPERTS, TOPK, 4096).reshape((N_PIPE, MICRO, TOKENS, TOPK))
    route_weights = jnp.clip(0.2 + 0.8 * jax.random.uniform(key_list[3], (N_PIPE, MICRO, TOKENS, TOPK), jnp.float32) ** steps_of(key_list[3], (N_PIPE, MICRO, TOKENS, TOPK), ((0, 8), (2, 8)), -0.2, 0.2), 0.2, 1.0)
    picks = jax.vmap(lambda own: jax.random.permutation(own, TOK_DEV))(jax.random.split(key_list[4], N_PIPE * MICRO * N_EXPERT)).reshape((N_PIPE, MICRO, N_EXPERT, TOK_DEV)).astype(jnp.int32)
    w_gate = gaussian(key_list[5], (N_PIPE, EXPERTS, D, FF), D ** -0.5, 0.09375, ((0, 8), (1, 8), (3, 4)))
    w_up = gaussian(key_list[6], (N_PIPE, EXPERTS, D, FF), D ** -0.5, 0.09375, ((0, 8), (1, 8), (3, 4)))
    w_down = gaussian(key_list[7], (N_PIPE, EXPERTS, FF, D), FF ** -0.5, 0.15625, ((0, 8), (1, 8), (2, 4)))
    return dict(tokens=tokens, gains=gains, route_ids=route_ids, route_weights=route_weights, picks=picks, w_gate=w_gate, w_up=w_up, w_down=w_down)


epsilon = 1e-06

def find_slots(ordered_ids, capacity):
    onehot = (ordered_ids[..., None] == jnp.arange(EXPERTS, dtype=jnp.int32)).astype(jnp.int32)
    earlier = jnp.cumsum(onehot, axis=-2) - onehot
    slot_index = lax.optimization_barrier(jnp.sum(earlier * onehot, axis=-1))
    return (slot_index, slot_index < capacity)

def expert_ffn(operands):
    row_block, gate_matrix, up_matrix, down_matrix = operands
    gate_val = jnp.dot(row_block, gate_matrix, preferred_element_type=jnp.float32)
    up_val = jnp.dot(row_block, up_matrix, preferred_element_type=jnp.float32)
    hidden = (jax.nn.silu(gate_val) * up_val).astype(jnp.bfloat16)
    shard_width = FF // N_TENSOR
    summed = jnp.zeros((row_block.shape[0], D), jnp.float32)
    for shard_index in range(N_TENSOR):
        lower = shard_index * shard_width
        partial_sum = jnp.dot(hidden[:, lower:lower + shard_width], down_matrix[lower:lower + shard_width], preferred_element_type=jnp.float32)
        rounded = lax.optimization_barrier(partial_sum.astype(jnp.bfloat16))
        summed = summed + rounded.astype(jnp.float32)
    return summed.astype(jnp.bfloat16)

def moe_section(stream, gain_row, section_ids, section_weights, section_picks, gate_all, up_all, down_all):
    groups = N_EXPERT
    offsets = (jnp.arange(groups, dtype=jnp.int32) * TOK_DEV)[:, None]
    ordered = (section_picks + offsets).astype(jnp.int32).reshape(groups, N_TENSOR, QUARTER)
    stream_f = stream.astype(jnp.float32)
    inv_rms = lax.rsqrt(lax.optimization_barrier(jnp.mean(stream_f * stream_f, axis=1, keepdims=True)) + epsilon)
    normed = (stream_f * inv_rms * gain_row[None, :]).astype(jnp.bfloat16)
    ordered_ids = section_ids[ordered].reshape(groups, N_TENSOR, QUARTER * TOPK)
    ordered_weights = section_weights[ordered].reshape(groups, N_TENSOR, QUARTER * TOPK)
    slot_index, kept_mask = find_slots(ordered_ids, CAP)
    route_tokens = jnp.repeat(ordered, TOPK, axis=2)
    group_index = jnp.arange(groups, dtype=jnp.int32)[:, None, None]
    rank_index = jnp.arange(N_TENSOR, dtype=jnp.int32)[None, :, None]
    position = ((ordered_ids * groups + group_index) * N_TENSOR + rank_index) * CAP + slot_index
    filled = EXPERTS * groups * N_TENSOR * CAP
    target = jnp.where(kept_mask, position, filled).astype(jnp.int32)
    source = jnp.full((filled + 1,), TOKENS, jnp.int32).at[target.reshape(-1)].set(route_tokens.reshape(-1))
    padded = jnp.concatenate([normed, jnp.zeros((1, D), jnp.bfloat16)], axis=0)
    row_block = padded[source[:filled]].reshape(EXPERTS, groups * N_TENSOR * CAP, D)
    results = lax.map(expert_ffn, (row_block, gate_all, up_all, down_all))
    flat_results = jnp.concatenate([results.reshape(filled, D), jnp.zeros((1, D), jnp.bfloat16)], axis=0)
    picked = flat_results[target].astype(jnp.float32)
    weighted = picked * (ordered_weights * kept_mask)[..., None]
    update = lax.optimization_barrier(jnp.sum(weighted.reshape(groups, N_TENSOR, QUARTER, TOPK, D), axis=3))
    stream_new = stream_f.at[ordered.reshape(-1)].add(update.reshape(-1, D))
    return stream_new.astype(jnp.bfloat16)

def reference(tokens, gains, route_ids, route_weights, picks, w_gate, w_up, w_down):
    finished = []
    for micro_index in range(MICRO):
        stream = tokens[micro_index]
        column = []
        for section_index in range(N_PIPE):
            stream = moe_section(stream, gains[section_index], route_ids[section_index, micro_index], route_weights[section_index, micro_index], picks[section_index, micro_index], w_gate[section_index], w_up[section_index], w_down[section_index])
            column.append(stream)
        finished.append(jnp.stack(column))
    return jnp.stack(finished, axis=1)
```

```python
import functools

import jax
import jax.numpy as jnp
from jax import lax
from jax.experimental import pallas as pl
from jax.experimental.pallas import tpu as pltpu
from jax.sharding import PartitionSpec as P

epsilon = 1e-06
MESH = pl.DeviceIdType.MESH
F32 = jnp.float32
BF16 = jnp.bfloat16
CH = 4
MAIN = 16
REM = 4
BLOCK = CH * (MAIN + REM)


def layer_kernel(
    sizes, tokens, gains, meta, weights, w_gate, w_up, w_down, out,
    nmeta, placing, comb, perm, h_in, fresh, isend, dsend, x, wgu, wdt, acc, sq, hid, yacc, zsend, ret,
    w_sem, wt_send, wt_recv, m_send, m_recv, h_loc, h_send, h_recv, i_send, d_send, d_recv,
    a_send, a_recv, b_send, b_recv, hs_send, hs_recv, hf_send, hf_recv, z_send, z_recv,
):
    micros, n_p, n_t, n_e, capacity, toks, width = sizes
    n_hi = n_e // 2
    lanes = width // CH
    rows = n_e * (MAIN + REM)
    main_rows = n_e * MAIN
    p = lax.axis_index("pipe")
    r = lax.axis_index("tensor")
    z = lax.axis_index("expert")
    z_hi = lax.div(z, 2)
    core = lax.rem(z, 2)
    right = lax.rem(r + 1, n_t)
    left = lax.rem(r + n_t - 1, n_t)
    across_r = lax.rem(r + 2, n_t)

    def diff(j, odd):
        return [0, 1 + 2 * odd, 3 - 2 * odd, 2][j]

    def target(k, odd):
        hi = lax.rem(z_hi + diff(k // 2, odd), n_hi)
        return 2 * hi + (core if k % 2 == 0 else 1 - core)

    def source(k, odd):
        hi = lax.rem(z_hi - diff(k // 2, odd) + n_hi, n_hi)
        return 2 * hi + (core if k % 2 == 0 else 1 - core)

    def remote(src, dst, ssem, rsem, where):
        return pltpu.make_async_remote_copy(
            src_ref=src, dst_ref=dst, send_sem=ssem, recv_sem=rsem,
            device_id=where, device_id_type=MESH,
        )

    def cols_of(q, size):
        return pl.ds(pl.multiple_of(q * size, size), size)

    hidden_width = w_gate.shape[3]
    loads = [
        pltpu.make_async_copy(w_gate.at[0, 0], wgu.at[:, :hidden_width], w_sem.at[0]),
        pltpu.make_async_copy(w_up.at[0, 0], wgu.at[:, hidden_width:], w_sem.at[1]),
        pltpu.make_async_copy(w_down.at[0, 0, :, cols_of(r, width)], wdt.at[r], w_sem.at[2]),
    ]

    def first_load(m, c):
        cols = pl.ds(pl.multiple_of(r * width + c * lanes, lanes), lanes)
        return pltpu.make_async_copy(
            tokens.at[m, :, cols], h_in.at[m, c * toks:(c + 1) * toks], h_loc.at[m, c])

    @pl.when(p == 0)
    def _():
        for m in range(micros):
            for c in range(CH):
                first_load(m, c).start()

    for load in loads:
        load.start()

    barrier = pltpu.get_barrier_semaphore()

    def greet(where):
        pl.semaphore_signal(barrier, inc=1, device_id=where, device_id_type=MESH)

    for d in range(1, n_e):
        greet({"expert": lax.rem(z + d, n_e)})
    for d in range(1, n_t):
        greet({"tensor": lax.rem(r + d, n_t)})

    @pl.when(p > 0)
    def _():
        for e in range(n_e):
            greet({"pipe": p - 1, "expert": e})

    @pl.when(p < n_p - 1)
    def _():
        for e in range(n_e):
            greet({"pipe": p + 1, "expert": e})

    def iota(shape, dim):
        return lax.broadcasted_iota(jnp.int32, shape, dim)

    down = iota((toks, toks), 0)
    across = iota((toks, toks), 1)
    same = down == across
    quarter = toks // n_t

    def column(row):
        return jnp.sum(jnp.where(same, row, jnp.zeros_like(row)), axis=1, keepdims=True)

    def row_of(col):
        return jnp.sum(jnp.where(same, col, jnp.zeros_like(col)), axis=0, keepdims=True)

    def slots(table, m):
        pos = jnp.sum(jnp.where(table[m, 2:3, :toks] == down, across, 0), axis=1, keepdims=True)
        pos_row = row_of(pos)
        block = lax.div(pos, quarter)
        before = (lax.div(pos_row, quarter) == block) & (pos_row < pos)
        found = []
        for e in range(n_e):
            named = jnp.zeros((1, toks), jnp.int32)
            for k in range(2):
                named = named + jnp.where(table[m, k:k + 1, :toks] == e, 1, 0)
            slot = jnp.sum(jnp.where(before, named, 0), axis=1, keepdims=True)
            kept = (column(named) > 0) & (slot < capacity)
            found.append(jnp.where(kept, block * capacity + slot, -1))
        return found

    def place(table, m):
        i = iota((BLOCK, CH * toks), 0)
        is_main = i < CH * MAIN
        key = jnp.where(
            is_main,
            lax.rem(i, MAIN) + 32 * lax.div(i, MAIN),
            MAIN + lax.rem(i, REM) + 32 * lax.div(i - CH * MAIN, REM))
        t_of = lax.rem(iota((toks, CH * toks), 1), toks) == iota((toks, CH * toks), 0)
        shift = 32 * lax.div(iota((1, CH * toks), 1), toks)
        for e, col in enumerate(slots(table, m)):
            wide = jnp.sum(jnp.where(t_of, col, 0), axis=0, keepdims=True) + shift
            placing[m, e] = jnp.where(key == wide, 1.0, 0.0).astype(BF16)

    def weigh(m):
        shape = (toks, 2 * main_rows)
        i = iota(shape, 1)
        is_main = i < main_rows
        of = jnp.where(is_main, lax.div(i, MAIN), lax.div(i - main_rows, CH * REM))
        slot = jnp.where(is_main, lax.rem(i, MAIN), MAIN + lax.rem(i, REM))
        chunk = lax.div(lax.rem(i, CH * REM), REM)
        key = of * 32 + slot
        total = jnp.zeros(shape, F32)
        for e, col in enumerate(slots(meta, m)):
            w_row = jnp.zeros((1, toks), F32)
            for k in range(2):
                w_row = w_row + jnp.where(meta[m, k:k + 1, :toks] == e, weights[m, k:k + 1], 0.0)
            wanted = jnp.where(col < 0, -1, col + 32 * e)
            total = total + jnp.where(key == wanted, column(w_row), 0.0)
        for c in range(CH):
            part = jnp.where(is_main | (chunk == c), total, 0.0)
            high = part.astype(BF16)
            comb[m, c, :toks] = high
            comb[m, c, toks:] = (part - high.astype(F32)).astype(BF16)

    def make_perm():
        n = n_e * CH * REM
        i = iota((n, n), 0)
        j = iota((n, n), 1)
        per = n_e * REM
        there = lax.div(lax.rem(i, per), REM) * (CH * REM) + lax.div(i, per) * REM + lax.rem(i, REM)
        back = lax.div(lax.rem(i, CH * REM), REM) * per + lax.div(i, CH * REM) * REM + lax.rem(i, REM)
        perm[0] = jnp.where(j == there, 1.0, 0.0).astype(BF16)
        perm[1] = jnp.where(j == back, 1.0, 0.0).astype(BF16)

    @pl.when(p == 0)
    def _():
        place(meta, 0)

    ends = jnp.where(p > 0, n_e, 0) + jnp.where(p < n_p - 1, n_e, 0)
    pl.semaphore_wait(barrier, n_e - 1 + n_t - 1 + ends)

    def meta_copy():
        return remote(meta, nmeta, m_send.at[0], m_recv.at[0], {"pipe": jnp.maximum(p - 1, 0)})

    def wt_copy(d):
        there = lax.rem(r + d, n_t)
        return remote(w_down.at[0, 0, :, cols_of(there, width)], wdt.at[r],
                      wt_send.at[d - 1], wt_recv.at[d - 1], {"tensor": there})

    def relay(m):
        return remote(fresh.at[m], h_in.at[m], h_send.at[m], h_recv.at[m],
                      {"pipe": jnp.minimum(p + 1, n_p - 1)})

    def i_copy(m, k):
        e = target(k, 0)
        return remote(isend.at[m, e], x.at[m, r, z], i_send.at[m, k], d_recv.at[m, k], {"expert": e})

    def d_copy(m, k):
        e = target(k, lax.rem(p + 1, 2))
        return remote(dsend.at[m, e], x.at[m, r, z], d_send.at[m, k], d_recv.at[m, k],
                      {"pipe": jnp.minimum(p + 1, n_p - 1), "expert": e})

    def a_copy(m, way, k):
        block = x.at[m, r, source(k, lax.rem(p, 2))]
        return remote(block, block, a_send.at[m, way, k], a_recv.at[m, way, k],
                      {"tensor": left if way else right})

    def b_copy(m, k):
        block = x.at[m, right if k % 2 else left, source(k, lax.rem(p, 2))]
        return remote(block, block, b_send.at[m, k], b_recv.at[m, k],
                      {"tensor": left if k % 2 else right})

    half = rows // 2

    def hs_copy(m, way, k):
        block = hid.at[m, r, k * half:(k + 1) * half]
        return remote(block, block, hs_send.at[m, way, k], hs_recv.at[m, way, k],
                      {"tensor": left if way else right})

    def hf_copy(m, k):
        block = hid.at[m, right if k else left, k * half:(k + 1) * half]
        return remote(block, block, hf_send.at[m, k], hf_recv.at[m, k],
                      {"tensor": left if k else right})

    def z_copy(m, k):
        e = target(k, 0)
        return remote(zsend.at[m, e], ret.at[m, z], z_send.at[m, k], z_recv.at[m, k], {"expert": e})

    def route(m, src, dst, odd, copy):
        h = src[m]
        for j in range(n_hi):
            hi = lax.rem(z_hi + diff(j, odd), n_hi)
            pair = pl.ds(2 * hi, 2)
            both = jnp.dot(placing[m, pair].reshape(2 * BLOCK, CH * toks), h, preferred_element_type=F32)
            dst[m, pair] = both.astype(BF16).reshape(2, BLOCK, lanes)
            for k in (2 * j, 2 * j + 1):
                if copy is i_copy and k == 0:
                    x[m, r, z] = dst[m, z]
                else:
                    copy(m, k).start()

    def own(m, k):
        if k == 0:
            @pl.when(p > 0)
            def _():
                d_copy(m, k).wait_recv()
        else:
            d_copy(m, k).wait_recv()
        for way in range(2):
            a_copy(m, way, k).start()

    def forward(m, k):
        a_copy(m, k % 2, k).wait_recv()
        b_copy(m, k).start()

    def gather_rest(m):
        for k in range(n_e):
            a_copy(m, 1 - k % 2, k).wait_recv()

    def gather_far(m):
        for k in range(n_e):
            b_copy(m, k).wait_recv()

    def project(m, q, first):
        rem = jnp.dot(perm[0], x[m, q, :, CH * MAIN:BLOCK, :].reshape(main_rows, lanes),
                      preferred_element_type=F32)
        per = n_e * REM
        parts = []
        squares = None
        for c in range(CH):
            body = x[m, q, :, c * MAIN:(c + 1) * MAIN, :].reshape(main_rows, lanes).astype(F32)
            full = jnp.concatenate([body, rem[c * per:(c + 1) * per]], axis=0)
            squares = full * full if squares is None else squares + full * full
            parts.append((full * gains[q * CH + c]).astype(BF16))
        both = jnp.dot(jnp.concatenate(parts, axis=1), wgu[cols_of(q, width), :],
                       preferred_element_type=F32)
        if first:
            acc[...] = both
            sq[...] = squares
        else:
            acc[...] += both
            sq[...] += squares

    def hide(m):
        inv = lax.rsqrt(jnp.sum(sq[...], axis=1, keepdims=True) * (1.0 / (n_t * width)) + epsilon)
        gate = acc[:, :hidden_width] * inv
        up = acc[:, hidden_width:] * inv
        hid[m, r] = (gate / (1.0 + jnp.exp(-gate)) * up).astype(BF16)
        for way, k in ((0, 0), (1, 1), (0, 1), (1, 0)):
            hs_copy(m, way, k).start()

    def hid_forward(m):
        for k in range(2):
            hs_copy(m, k, k).wait_recv()
            hf_copy(m, k).start()

    def lower(m, q, first):
        part = jnp.dot(hid[m, q], wdt[q], preferred_element_type=F32)
        if first:
            yacc[...] = part
        else:
            yacc[...] += part

    def give_back(m):
        rem = []
        for c in range(CH):
            part = yacc[:, c * lanes:(c + 1) * lanes].astype(BF16)
            zsend[m, :, c * MAIN:(c + 1) * MAIN, :] = part[:main_rows].reshape(n_e, MAIN, lanes)
            rem.append(part[main_rows:])
        swapped = jnp.dot(perm[1], jnp.concatenate(rem, axis=0), preferred_element_type=F32)
        zsend[m, :, CH * MAIN:BLOCK, :] = swapped.astype(BF16).reshape(n_e, CH * REM, lanes)
        for k in range(n_e - 1, 0, -1):
            z_copy(m, k).start()
        ret[m, z] = zsend[m, z]

    def combine(m):
        @pl.when(p > 0)
        def _():
            relay(m).wait_recv()
        for k in range(1, n_e):
            z_copy(m, k).wait_recv()
        last = ret[m, :, CH * MAIN:BLOCK, :].reshape(main_rows, lanes)
        for c in range(CH):
            got = jnp.concatenate(
                [ret[m, :, c * MAIN:(c + 1) * MAIN, :].reshape(main_rows, lanes), last], axis=0)
            both = jnp.dot(comb[m, c], got, preferred_element_type=F32)
            span = slice(c * toks, (c + 1) * toks)
            new = (h_in[m, span].astype(F32) + (both[:toks] + both[toks:])).astype(BF16)
            fresh[m, span] = new
            out[0, m, :, c * lanes:(c + 1) * lanes] = new

        @pl.when(p < n_p - 1)
        def _():
            route(m, fresh, dsend, lax.rem(p + 1, 2), d_copy)
            relay(m).start()

    @pl.when(p == 0)
    def _():
        for m in range(micros):
            if m:
                place(meta, m)
            for c in range(CH):
                first_load(m, c).wait()
            route(m, h_in, isend, 0, i_copy)

    @pl.when(p > 0)
    def _():
        meta_copy().start()

    for d in (1, 3, 2):
        wt_copy(d).start()
    make_perm()
    for m in range(micros):
        weigh(m)

    @pl.when(p < n_p - 1)
    def _():
        meta_copy().wait_recv()
        for m in range(micros):
            place(nmeta, m)

    for m in range(micros):
        for k in range(4):
            own(m, k)
        for k in range(4):
            own(m, k + 4)
            forward(m, k)
        if m == 0:
            loads[0].wait()
            loads[1].wait()
        project(m, r, True)
        for k in range(4, n_e):
            forward(m, k)
        gather_rest(m)
        project(m, left, False)
        project(m, right, False)
        gather_far(m)
        project(m, across_r, False)
        hide(m)
        if m == 0:
            loads[2].wait()
        lower(m, r, True)
        hid_forward(m)
        hs_copy(m, 0, 1).wait_recv()
        hs_copy(m, 1, 0).wait_recv()
        if m == 0:
            for d in (1, 3, 2):
                wt_copy(d).wait_recv()
        lower(m, left, False)
        lower(m, right, False)
        for k in range(2):
            hf_copy(m, k).wait_recv()
        lower(m, across_r, False)
        give_back(m)
        combine(m)

    for d in (1, 3, 2):
        wt_copy(d).wait_send()

    @pl.when(p > 0)
    def _():
        meta_copy().wait_send()

    for m in range(micros):
        for k in range(n_e):
            for way in range(2):
                a_copy(m, way, k).wait_send()
            b_copy(m, k).wait_send()
            if k:
                z_copy(m, k).wait_send()
        for k in range(2):
            for way in range(2):
                hs_copy(m, way, k).wait_send()
            hf_copy(m, k).wait_send()

        @pl.when(p == 0)
        def _():
            for k in range(1, n_e):
                i_copy(m, k).wait_send()

        @pl.when(p < n_p - 1)
        def _():
            for k in range(n_e):
                d_copy(m, k).wait_send()
            relay(m).wait_send()


def local(mesh_shape, tokens, gains, route_ids, route_weights, picks, w_gate, w_up, w_down):
    n_p, n_t, n_e = mesh_shape
    micros, toks, model_width = tokens.shape
    route_count = route_ids.shape[3]
    quarter = toks // n_t
    capacity = 4 * quarter * route_count // (3 * n_e)
    width = model_width // n_t
    lanes = width // CH
    hidden_width = w_gate.shape[3]
    rows = n_e * (MAIN + REM)
    ids = route_ids[0].transpose(0, 2, 1)
    weights = route_weights[0].transpose(0, 2, 1)
    meta = jnp.concatenate([ids, picks[0]], axis=1)
    meta = jnp.pad(meta, ((0, 0), (0, 8 - meta.shape[1]), (0, 128 - toks)))
    gain_rows = gains.reshape(n_t * CH, 1, lanes)

    sizes = (micros, n_p, n_t, n_e, capacity, toks, width)
    dma = pltpu.SemaphoreType.DMA
    vmem = pl.BlockSpec(memory_space=pltpu.VMEM)
    anywhere = pl.BlockSpec(memory_space=pl.ANY)
    return pl.pallas_call(
        functools.partial(layer_kernel, sizes),
        out_shape=jax.ShapeDtypeStruct((1, micros, toks, width), BF16),
        in_specs=[anywhere, vmem, vmem, vmem, anywhere, anywhere, anywhere],
        out_specs=vmem,
        scratch_shapes=[
            pltpu.VMEM(meta.shape, jnp.int32),
            pltpu.VMEM((micros, n_e, BLOCK, CH * toks), BF16),
            pltpu.VMEM((micros, CH, 2 * toks, 2 * n_e * MAIN), BF16),
            pltpu.VMEM((2, n_e * CH * REM, n_e * CH * REM), BF16),
            pltpu.VMEM((micros, CH * toks, lanes), BF16),
            pltpu.VMEM((micros, CH * toks, lanes), BF16),
            pltpu.VMEM((micros, n_e, BLOCK, lanes), BF16),
            pltpu.VMEM((micros, n_e, BLOCK, lanes), BF16),
            pltpu.VMEM((micros, n_t, n_e, BLOCK, lanes), BF16),
            pltpu.VMEM((model_width, 2 * hidden_width), BF16),
            pltpu.VMEM((n_t, hidden_width, width), BF16),
            pltpu.VMEM((rows, 2 * hidden_width), F32),
            pltpu.VMEM((rows, lanes), F32),
            pltpu.VMEM((micros, n_t, rows, hidden_width), BF16),
            pltpu.VMEM((rows, width), F32),
            pltpu.VMEM((micros, n_e, BLOCK, lanes), BF16),
            pltpu.VMEM((micros, n_e, BLOCK, lanes), BF16),
            dma((3,)), dma((3,)), dma((3,)), dma((1,)), dma((1,)),
            dma((micros, CH)), dma((micros,)), dma((micros,)),
            dma((micros, n_e)), dma((micros, n_e)), dma((micros, n_e)),
            dma((micros, 2, n_e)), dma((micros, 2, n_e)), dma((micros, n_e)), dma((micros, n_e)),
            dma((micros, 2, 2)), dma((micros, 2, 2)), dma((micros, 2)), dma((micros, 2)),
            dma((micros, n_e)), dma((micros, n_e)),
        ],
        compiler_params=pltpu.CompilerParams(
            collective_id=0, has_side_effects=True, vmem_limit_bytes=67043328 - 600 * 1024
        ),
    )(tokens, gain_rows, meta, weights, w_gate, w_up, w_down)


def solution(mesh):
    mesh_shape = (mesh.shape["pipe"], mesh.shape["tensor"], mesh.shape["expert"])
    return jax.shard_map(
        functools.partial(local, mesh_shape),
        mesh=mesh,
        in_specs=(
            P(None, "expert", None),
            P("pipe", None),
            P("pipe", None, "expert", None),
            P("pipe", None, "expert", None),
            P("pipe", None, "expert", None),
            P("pipe", "expert", None, "tensor"),
            P("pipe", "expert", None, "tensor"),
            P("pipe", "expert", "tensor", None),
        ),
        out_specs=P("pipe", None, "expert", "tensor"),
        check_vma=False,
    )
```

```python
import functools

import jax
import jax.numpy as jnp
from jax import lax
from jax.experimental import pallas as pl
from jax.experimental.pallas import tpu as pltpu
from jax.sharding import PartitionSpec as P

epsilon = 1e-06
MESH = pl.DeviceIdType.MESH
F32 = jnp.float32
BF16 = jnp.bfloat16
CH = 4
MAIN = 16
REM = 4
SHARE = 160
PIECES = 2
HELPERS = (2, 6)
BLOCK = CH * (MAIN + REM)


def layer_kernel(
    sizes, tokens, gains, meta, weights, w_gate, w_up, w_down, out,
    nmeta, placing, comb, perm, h_in, fresh, isend, dsend, x, wgu, wdt, acc, sq, hid, yacc, bounce, zsend, ret,
    w_sem, wt_send, wt_recv, m_send, m_recv, h_loc, h_send, h_recv, i_send, d_send, d_recv,
    a_send, a_recv, b_send, b_recv, hs_send, hs_recv, hf_send, hf_recv, u_send, u_recv, v_send, v_recv, z_send, z_recv,
):
    micros, n_p, n_t, n_e, capacity, toks, width = sizes
    n_hi = n_e // 2
    lanes = width // CH
    rows = n_e * (MAIN + REM)
    main_rows = n_e * MAIN
    p = lax.axis_index("pipe")
    r = lax.axis_index("tensor")
    z = lax.axis_index("expert")
    z_hi = lax.div(z, 2)
    core = lax.rem(z, 2)
    right = lax.rem(r + 1, n_t)
    left = lax.rem(r + n_t - 1, n_t)
    across_r = lax.rem(r + 2, n_t)

    def diff(j, odd):
        return [0, 1 + 2 * odd, 3 - 2 * odd, 2][j]

    def target(k, odd):
        hi = lax.rem(z_hi + diff(k // 2, odd), n_hi)
        return 2 * hi + (core if k % 2 == 0 else 1 - core)

    def source(k, odd):
        hi = lax.rem(z_hi - diff(k // 2, odd) + n_hi, n_hi)
        return 2 * hi + (core if k % 2 == 0 else 1 - core)

    def remote(src, dst, ssem, rsem, where):
        return pltpu.make_async_remote_copy(
            src_ref=src, dst_ref=dst, send_sem=ssem, recv_sem=rsem,
            device_id=where, device_id_type=MESH,
        )

    def cols_of(q, size):
        return pl.ds(pl.multiple_of(q * size, size), size)

    hidden_width = w_gate.shape[3]
    loads = [
        pltpu.make_async_copy(w_gate.at[0, 0], wgu.at[:, :hidden_width], w_sem.at[0]),
        pltpu.make_async_copy(w_up.at[0, 0], wgu.at[:, hidden_width:], w_sem.at[1]),
        pltpu.make_async_copy(w_down.at[0, 0, :, cols_of(r, width)], wdt.at[r], w_sem.at[2]),
    ]

    def first_load(m, c):
        cols = pl.ds(pl.multiple_of(r * width + c * lanes, lanes), lanes)
        return pltpu.make_async_copy(
            tokens.at[m, :, cols], h_in.at[m, c * toks:(c + 1) * toks], h_loc.at[m, c])

    @pl.when(p == 0)
    def _():
        for m in range(micros):
            for c in range(CH):
                first_load(m, c).start()

    for load in loads:
        load.start()

    barrier = pltpu.get_barrier_semaphore()

    def greet(where):
        pl.semaphore_signal(barrier, inc=1, device_id=where, device_id_type=MESH)

    for d in range(1, n_e):
        greet({"expert": lax.rem(z + d, n_e)})
    for d in range(1, n_t):
        greet({"tensor": lax.rem(r + d, n_t)})

    @pl.when(p > 0)
    def _():
        for e in range(n_e):
            greet({"pipe": p - 1, "expert": e})

    @pl.when(p < n_p - 1)
    def _():
        for e in range(n_e):
            greet({"pipe": p + 1, "expert": e})

    @pl.when(p == 0)
    def _():
        for there in HELPERS:
            for d in range(n_t):
                greet({"pipe": there, "tensor": lax.rem(r + d, n_t)})

    helper = (p == HELPERS[0]) | (p == HELPERS[1])

    @pl.when(helper)
    def _():
        for d in range(n_t):
            greet({"pipe": 0, "tensor": lax.rem(r + d, n_t)})

    def iota(shape, dim):
        return lax.broadcasted_iota(jnp.int32, shape, dim)

    down = iota((toks, toks), 0)
    across = iota((toks, toks), 1)
    same = down == across
    quarter = toks // n_t

    def column(row):
        return jnp.sum(jnp.where(same, row, jnp.zeros_like(row)), axis=1, keepdims=True)

    def row_of(col):
        return jnp.sum(jnp.where(same, col, jnp.zeros_like(col)), axis=0, keepdims=True)

    def slots(table, m):
        pos = jnp.sum(jnp.where(table[m, 2:3, :toks] == down, across, 0), axis=1, keepdims=True)
        pos_row = row_of(pos)
        block = lax.div(pos, quarter)
        before = (lax.div(pos_row, quarter) == block) & (pos_row < pos)
        found = []
        for e in range(n_e):
            named = jnp.zeros((1, toks), jnp.int32)
            for k in range(2):
                named = named + jnp.where(table[m, k:k + 1, :toks] == e, 1, 0)
            slot = jnp.sum(jnp.where(before, named, 0), axis=1, keepdims=True)
            kept = (column(named) > 0) & (slot < capacity)
            found.append(jnp.where(kept, block * capacity + slot, -1))
        return found

    def place(table, m):
        i = iota((BLOCK, CH * toks), 0)
        is_main = i < CH * MAIN
        key = jnp.where(
            is_main,
            lax.rem(i, MAIN) + 32 * lax.div(i, MAIN),
            MAIN + lax.rem(i, REM) + 32 * lax.div(i - CH * MAIN, REM))
        t_of = lax.rem(iota((toks, CH * toks), 1), toks) == iota((toks, CH * toks), 0)
        shift = 32 * lax.div(iota((1, CH * toks), 1), toks)
        for e, col in enumerate(slots(table, m)):
            wide = jnp.sum(jnp.where(t_of, col, 0), axis=0, keepdims=True) + shift
            placing[m, e] = jnp.where(key == wide, 1.0, 0.0).astype(BF16)

    def weigh(m):
        shape = (toks, 2 * main_rows)
        i = iota(shape, 1)
        is_main = i < main_rows
        of = jnp.where(is_main, lax.div(i, MAIN), lax.div(i - main_rows, CH * REM))
        slot = jnp.where(is_main, lax.rem(i, MAIN), MAIN + lax.rem(i, REM))
        chunk = lax.div(lax.rem(i, CH * REM), REM)
        key = of * 32 + slot
        total = jnp.zeros(shape, F32)
        for e, col in enumerate(slots(meta, m)):
            w_row = jnp.zeros((1, toks), F32)
            for k in range(2):
                w_row = w_row + jnp.where(meta[m, k:k + 1, :toks] == e, weights[m, k:k + 1], 0.0)
            wanted = jnp.where(col < 0, -1, col + 32 * e)
            total = total + jnp.where(key == wanted, column(w_row), 0.0)
        for c in range(CH):
            part = jnp.where(is_main | (chunk == c), total, 0.0)
            high = part.astype(BF16)
            comb[m, c, :toks] = high
            comb[m, c, toks:] = (part - high.astype(F32)).astype(BF16)

    def make_perm():
        n = n_e * CH * REM
        i = iota((n, n), 0)
        j = iota((n, n), 1)
        per = n_e * REM
        there = lax.div(lax.rem(i, per), REM) * (CH * REM) + lax.div(i, per) * REM + lax.rem(i, REM)
        back = lax.div(lax.rem(i, CH * REM), REM) * per + lax.div(i, CH * REM) * REM + lax.rem(i, REM)
        perm[0] = jnp.where(j == there, 1.0, 0.0).astype(BF16)
        perm[1] = jnp.where(j == back, 1.0, 0.0).astype(BF16)

    @pl.when(p == 0)
    def _():
        place(meta, 0)

    ends = jnp.where(p > 0, n_e, 0) + jnp.where(p < n_p - 1, n_e, 0)
    ends = ends + jnp.where(p == 0, len(HELPERS) * n_t, 0) + jnp.where(helper, n_t, 0)
    pl.semaphore_wait(barrier, n_e - 1 + n_t - 1 + ends)

    def meta_copy():
        return remote(meta, nmeta, m_send.at[0], m_recv.at[0], {"pipe": jnp.maximum(p - 1, 0)})

    def wt_copy(d):
        there = lax.rem(r + d, n_t)
        return remote(w_down.at[0, 0, :, cols_of(there, width)], wdt.at[r],
                      wt_send.at[d - 1], wt_recv.at[d - 1], {"tensor": there})

    piece = SHARE // PIECES
    rest = hidden_width - len(HELPERS) * SHARE

    def u_copy(n, d, c):
        there = lax.rem(r + d, n_t)
        part = pl.ds(n * SHARE + c * piece, piece)
        return remote(w_down.at[0, 0, part, cols_of(there, width)],
                      bounce.at[d - 1, c * piece:(c + 1) * piece],
                      u_send.at[n, d - 1, c], u_recv.at[d - 1, c],
                      {"pipe": HELPERS[n], "tensor": there})

    def v_copy(n, d, c):
        part = pl.ds(pl.multiple_of(n * SHARE + c * piece, piece), piece)
        return remote(bounce.at[d - 1, c * piece:(c + 1) * piece],
                      wdt.at[lax.rem(r - d + n_t, n_t), part],
                      v_send.at[d - 1, c], v_recv.at[n, d - 1, c], {"pipe": 0})

    def t_copy(d):
        there = lax.rem(r + d, n_t)
        part = pl.ds(hidden_width - rest, rest)
        return remote(w_down.at[0, 0, part, cols_of(there, width)], wdt.at[r, part],
                      wt_send.at[d - 1], wt_recv.at[d - 1], {"tensor": there})

    helper_rank = jnp.where(p == HELPERS[0], 0, 1)

    def relay(m):
        return remote(fresh.at[m], h_in.at[m], h_send.at[m], h_recv.at[m],
                      {"pipe": jnp.minimum(p + 1, n_p - 1)})

    def i_copy(m, k):
        e = target(k, 0)
        return remote(isend.at[m, e], x.at[m, r, z], i_send.at[m, k], d_recv.at[m, k], {"expert": e})

    def d_copy(m, k):
        e = target(k, lax.rem(p + 1, 2))
        return remote(dsend.at[m, e], x.at[m, r, z], d_send.at[m, k], d_recv.at[m, k],
                      {"pipe": jnp.minimum(p + 1, n_p - 1), "expert": e})

    def pair_of(j):
        return pl.ds(2 * lax.rem(z_hi - diff(j, lax.rem(p, 2)) + n_hi, n_hi), 2)

    def a_copy(m, way, j):
        block = x.at[m, r, pair_of(j)]
        return remote(block, block, a_send.at[m, way, j], a_recv.at[m, way, j],
                      {"tensor": left if way else right})

    def b_copy(m, j):
        block = x.at[m, right if j % 2 else left, pair_of(j)]
        return remote(block, block, b_send.at[m, j], b_recv.at[m, j],
                      {"tensor": left if j % 2 else right})

    half = rows // 2

    def hs_copy(m, way, k):
        block = hid.at[m, r, k * half:(k + 1) * half]
        return remote(block, block, hs_send.at[m, way, k], hs_recv.at[m, way, k],
                      {"tensor": left if way else right})

    def hf_copy(m, k):
        block = hid.at[m, right if k else left, k * half:(k + 1) * half]
        return remote(block, block, hf_send.at[m, k], hf_recv.at[m, k],
                      {"tensor": left if k else right})

    def z_copy(m, k):
        e = target(k, 0)
        return remote(zsend.at[m, e], ret.at[m, z], z_send.at[m, k], z_recv.at[m, k], {"expert": e})

    def route(m, src, dst, odd, copy):
        h = src[m]
        for j in range(n_hi):
            hi = lax.rem(z_hi + diff(j, odd), n_hi)
            pair = pl.ds(2 * hi, 2)
            both = jnp.dot(placing[m, pair].reshape(2 * BLOCK, CH * toks), h, preferred_element_type=F32)
            dst[m, pair] = both.astype(BF16).reshape(2, BLOCK, lanes)
            for k in (2 * j, 2 * j + 1):
                if copy is i_copy and k == 0:
                    x[m, r, z] = dst[m, z]
                else:
                    copy(m, k).start()

    def own(m, j):
        if j == 0:
            @pl.when(p > 0)
            def _():
                d_copy(m, 0).wait_recv()
        else:
            d_copy(m, 2 * j).wait_recv()
        d_copy(m, 2 * j + 1).wait_recv()
        for way in range(2):
            a_copy(m, way, j).start()

    def forward(m, j):
        a_copy(m, j % 2, j).wait_recv()
        b_copy(m, j).start()

    def gather_rest(m):
        for j in range(n_hi):
            a_copy(m, 1 - j % 2, j).wait_recv()

    def gather_far(m):
        for j in range(n_hi):
            b_copy(m, j).wait_recv()

    def project(m, q, first):
        rem = jnp.dot(perm[0], x[m, q, :, CH * MAIN:BLOCK, :].reshape(main_rows, lanes),
                      preferred_element_type=F32)
        per = n_e * REM
        parts = []
        squares = None
        for c in range(CH):
            body = x[m, q, :, c * MAIN:(c + 1) * MAIN, :].reshape(main_rows, lanes).astype(F32)
            full = jnp.concatenate([body, rem[c * per:(c + 1) * per]], axis=0)
            squares = full * full if squares is None else squares + full * full
            parts.append((full * gains[q * CH + c]).astype(BF16))
        both = jnp.dot(jnp.concatenate(parts, axis=1), wgu[cols_of(q, width), :],
                       preferred_element_type=F32)
        if first:
            acc[...] = both
            sq[...] = squares
        else:
            acc[...] += both
            sq[...] += squares

    def hide(m):
        inv = lax.rsqrt(jnp.sum(sq[...], axis=1, keepdims=True) * (1.0 / (n_t * width)) + epsilon)
        gate = acc[:, :hidden_width] * inv
        up = acc[:, hidden_width:] * inv
        hid[m, r] = (gate / (1.0 + jnp.exp(-gate)) * up).astype(BF16)

    def hid_forward(m):
        for k in range(2):
            hs_copy(m, k, k).wait_recv()
            hf_copy(m, k).start()

    def lower(m, q, first):
        part = jnp.dot(hid[m, q], wdt[q], preferred_element_type=F32)
        if first:
            yacc[...] = part
        else:
            yacc[...] += part

    def give_back(m):
        rem = []
        for c in range(CH):
            part = yacc[:, c * lanes:(c + 1) * lanes].astype(BF16)
            zsend[m, :, c * MAIN:(c + 1) * MAIN, :] = part[:main_rows].reshape(n_e, MAIN, lanes)
            rem.append(part[main_rows:])
        swapped = jnp.dot(perm[1], jnp.concatenate(rem, axis=0), preferred_element_type=F32)
        zsend[m, :, CH * MAIN:BLOCK, :] = swapped.astype(BF16).reshape(n_e, CH * REM, lanes)
        for k in range(n_e - 1, 0, -1):
            z_copy(m, k).start()
        ret[m, z] = zsend[m, z]

    def combine(m):
        @pl.when(p > 0)
        def _():
            relay(m).wait_recv()
        for k in range(1, n_e):
            z_copy(m, k).wait_recv()
        last = ret[m, :, CH * MAIN:BLOCK, :].reshape(main_rows, lanes)
        for c in range(CH):
            got = jnp.concatenate(
                [ret[m, :, c * MAIN:(c + 1) * MAIN, :].reshape(main_rows, lanes), last], axis=0)
            both = jnp.dot(comb[m, c], got, preferred_element_type=F32)
            span = slice(c * toks, (c + 1) * toks)
            new = (h_in[m, span].astype(F32) + (both[:toks] + both[toks:])).astype(BF16)
            fresh[m, span] = new
            out[0, m, :, c * lanes:(c + 1) * lanes] = new

        @pl.when(p < n_p - 1)
        def _():
            route(m, fresh, dsend, lax.rem(p + 1, 2), d_copy)
            relay(m).start()

    @pl.when(p == 0)
    def _():
        for m in range(micros):
            if m:
                place(meta, m)
            for c in range(CH):
                first_load(m, c).wait()
            route(m, h_in, isend, 0, i_copy)

    @pl.when(p > 0)
    def _():
        meta_copy().start()

    @pl.when(p == 0)
    def _():
        for d in (1, 3, 2):
            for c in range(PIECES):
                for n in range(len(HELPERS)):
                    u_copy(n, d, c).start()

    @pl.when(helper)
    def _():
        for d in (1, 3, 2):
            for c in range(PIECES):
                u_copy(0, d, c).wait_recv()
                v_copy(helper_rank, d, c).start()

    @pl.when(p > 0)
    def _():
        for d in (1, 3, 2):
            wt_copy(d).start()

    make_perm()
    for m in range(micros):
        weigh(m)

    @pl.when(p < n_p - 1)
    def _():
        meta_copy().wait_recv()
        for m in range(micros):
            place(nmeta, m)

    def arrive(d):
        @pl.when(p > 0)
        def _():
            wt_copy(d).wait_recv()

        @pl.when(p == 0)
        def _():
            t_copy(d).wait_recv()
            for c in range(PIECES):
                for n in range(len(HELPERS)):
                    v_copy(n, d, c).wait_recv()

    def lower_gathered(m):
        for way, k in ((0, 0), (1, 1), (0, 1), (1, 0)):
            hs_copy(m, way, k).start()
        if m == 0:
            loads[2].wait()
        lower(m, r, True)
        hid_forward(m)
        hs_copy(m, 0, 1).wait_recv()
        hs_copy(m, 1, 0).wait_recv()
        if m == 0:
            arrive(1)
        lower(m, left, False)
        if m == 0:
            arrive(3)
        lower(m, right, False)
        for k in range(2):
            hf_copy(m, k).wait_recv()
        if m == 0:
            arrive(2)
        lower(m, across_r, False)

    def when(test, fn, *args):
        pl.when(test)(functools.partial(fn, *args))

    def head(m):
        own(m, 0)
        own(m, 1)
        own(m, 2)
        forward(m, 0)
        own(m, 3)
        forward(m, 1)

    def middle(m):
        if m == 0:
            loads[0].wait()
            loads[1].wait()
        project(m, r, True)
        forward(m, 2)
        forward(m, 3)

        if m == 0:
            @pl.when(p == 0)
            def _():
                for d in (1, 3, 2):
                    t_copy(d).start()

        gather_rest(m)
        project(m, left, False)
        project(m, right, False)
        gather_far(m)
        project(m, across_r, False)
        hide(m)
        lower_gathered(m)
        give_back(m)

    head(0)
    for m in range(micros):
        middle(m)
        if m + 1 < micros:
            head(m + 1)
        combine(m)

    @pl.when(p > 0)
    def _():
        meta_copy().wait_send()
        for d in (1, 3, 2):
            wt_copy(d).wait_send()

    @pl.when(p == 0)
    def _():
        for d in (1, 3, 2):
            t_copy(d).wait_send()
            for c in range(PIECES):
                for n in range(len(HELPERS)):
                    u_copy(n, d, c).wait_send()

    @pl.when(helper)
    def _():
        for d in (1, 3, 2):
            for c in range(PIECES):
                v_copy(helper_rank, d, c).wait_send()

    for m in range(micros):
        for j in range(n_hi):
            for way in range(2):
                a_copy(m, way, j).wait_send()
            b_copy(m, j).wait_send()
        for k in range(1, n_e):
            z_copy(m, k).wait_send()

        for k in range(2):
            for way in range(2):
                hs_copy(m, way, k).wait_send()
            hf_copy(m, k).wait_send()

        @pl.when(p == 0)
        def _():
            for k in range(1, n_e):
                i_copy(m, k).wait_send()

        @pl.when(p < n_p - 1)
        def _():
            for k in range(n_e):
                d_copy(m, k).wait_send()
            relay(m).wait_send()


def local(mesh_shape, tokens, gains, route_ids, route_weights, picks, w_gate, w_up, w_down):
    n_p, n_t, n_e = mesh_shape
    micros, toks, model_width = tokens.shape
    route_count = route_ids.shape[3]
    quarter = toks // n_t
    capacity = 4 * quarter * route_count // (3 * n_e)
    width = model_width // n_t
    lanes = width // CH
    hidden_width = w_gate.shape[3]
    rows = n_e * (MAIN + REM)
    ids = route_ids[0].transpose(0, 2, 1)
    weights = route_weights[0].transpose(0, 2, 1)
    meta = jnp.concatenate([ids, picks[0]], axis=1)
    meta = jnp.pad(meta, ((0, 0), (0, 8 - meta.shape[1]), (0, 128 - toks)))
    gain_rows = gains.reshape(n_t * CH, 1, lanes)

    sizes = (micros, n_p, n_t, n_e, capacity, toks, width)
    dma = pltpu.SemaphoreType.DMA
    vmem = pl.BlockSpec(memory_space=pltpu.VMEM)
    anywhere = pl.BlockSpec(memory_space=pl.ANY)
    return pl.pallas_call(
        functools.partial(layer_kernel, sizes),
        out_shape=jax.ShapeDtypeStruct((1, micros, toks, width), BF16),
        in_specs=[anywhere, vmem, vmem, vmem, anywhere, anywhere, anywhere],
        out_specs=vmem,
        scratch_shapes=[
            pltpu.VMEM(meta.shape, jnp.int32),
            pltpu.VMEM((micros, n_e, BLOCK, CH * toks), BF16),
            pltpu.VMEM((micros, CH, 2 * toks, 2 * n_e * MAIN), BF16),
            pltpu.VMEM((2, n_e * CH * REM, n_e * CH * REM), BF16),
            pltpu.VMEM((micros, CH * toks, lanes), BF16),
            pltpu.VMEM((micros, CH * toks, lanes), BF16),
            pltpu.VMEM((micros, n_e, BLOCK, lanes), BF16),
            pltpu.VMEM((micros, n_e, BLOCK, lanes), BF16),
            pltpu.VMEM((micros, n_t, n_e, BLOCK, lanes), BF16),
            pltpu.VMEM((model_width, 2 * hidden_width), BF16),
            pltpu.VMEM((n_t, hidden_width, width), BF16),
            pltpu.VMEM((rows, 2 * hidden_width), F32),
            pltpu.VMEM((rows, lanes), F32),
            pltpu.VMEM((micros, n_t, rows, hidden_width), BF16),
            pltpu.VMEM((rows, width), F32),
            pltpu.VMEM((n_t - 1, SHARE, width), BF16),
            pltpu.VMEM((micros, n_e, BLOCK, lanes), BF16),
            pltpu.VMEM((micros, n_e, BLOCK, lanes), BF16),
            dma((3,)), dma((3,)), dma((3,)), dma((1,)), dma((1,)),
            dma((micros, CH)), dma((micros,)), dma((micros,)),
            dma((micros, n_e)), dma((micros, n_e)), dma((micros, n_e)),
            dma((micros, 2, n_e // 2)), dma((micros, 2, n_e // 2)), dma((micros, n_e // 2)), dma((micros, n_e // 2)),
            dma((micros, 2, 2)), dma((micros, 2, 2)), dma((micros, 2)), dma((micros, 2)),
            dma((2, n_t - 1, PIECES)), dma((n_t - 1, PIECES)), dma((n_t - 1, PIECES)), dma((2, n_t - 1, PIECES)),
            dma((micros, n_e)), dma((micros, n_e)),
        ],
        compiler_params=pltpu.CompilerParams(
            collective_id=0, has_side_effects=True, vmem_limit_bytes=67043328 - 600 * 1024
        ),
    )(tokens, gain_rows, meta, weights, w_gate, w_up, w_down)


def solution(mesh):
    mesh_shape = (mesh.shape["pipe"], mesh.shape["tensor"], mesh.shape["expert"])
    return jax.shard_map(
        functools.partial(local, mesh_shape),
        mesh=mesh,
        in_specs=(
            P(None, "expert", None),
            P("pipe", None),
            P("pipe", None, "expert", None),
            P("pipe", None, "expert", None),
            P("pipe", None, "expert", None),
            P("pipe", "expert", None, "tensor"),
            P("pipe", "expert", None, "tensor"),
            P("pipe", "expert", "tensor", None),
        ),
        out_specs=P("pipe", None, "expert", "tensor"),
        check_vma=False,
    )
```
